32 devices in a mesh: wave: 8 (over z, y), lev: 4 (over x, core).
Axes of the slice: x: 2, y: 2, z: 4, core: 2. Of those that a mesh axis runs over, the one named last changes fastest.
Arguments:
- spectral: bfloat16 [32, 6, 64, 1280], P('wave', None, 'lev'), may hold values from -0.01171875 to 0.01171875
- legendre: bfloat16 [32, 640, 1280], P('wave'), may hold values from -4 to 4
- wave_ids: int32 [32], replicated, may hold values from 0 to 1279, as said below
- trunc_lengths: int32 [32], replicated, may hold values from 1 to 1280, as said below
- cycle_points: int32 [1280], replicated, may hold values from 20 to 2560, as said below
- grid_coef: float32 [1280, 2560], P('wave'), may hold values from -6 to 6
- cycle_weights: float32 [640], replicated, may hold values from 0.1 to 2
- modes_in: bfloat16 [64, 64], replicated, may hold values from -0.75 to 0.75
- modes_out: bfloat16 [64, 64], replicated, may hold values from -0.75 to 0.75
- depths: float32 [64], replicated, may hold values from 0.05 to 20
Outputs:
- update: bfloat16 [32, 6, 64, 1280], P('wave', None, 'lev')
The draws below stay inside these ranges and needn't reach their ends.
Inputs may be any that keep to these rules, and one draw needn't show every extreme that they name: `wave_ids`: distinct zonal wavenumbers; one slot holds wavenumber 0. `trunc_lengths`: the length of slot m is at most 1280 minus wave_ids[m] and at least half of that; the slot of wavenumber 0 has length 1280. `cycle_points`: multiples of 4; cycle j and cycle 1280 - 1-j have the same count; cycles near the equator have 2560.
All inputs are finite; a program needn't handle non-finite values.
Results may differ from the reference program's by a relative error of at most 0.011.
Values may be sent and summed in bfloat16 or wider, within the bound.
A program may use at most 128 MiB of HBM per device.

```python
import math
import jax
import jax.numpy as jnp
from jax import lax

NT = 1280
NLAT = 1280
NHALF = 640
LONMAX = 2560
FIELDS = 3
M_WIN = 32
LEVELS = 64


def wave_table(key):
    base_key = jax.random.fold_in(key, 11)
    others = jax.random.permutation(jax.random.fold_in(base_key, 1), NT - 1)[:M_WIN - 1] + 1
    chosen = jnp.concatenate([jnp.zeros((1,), jnp.int32), others.astype(jnp.int32)])
    shuffle = jax.random.permutation(jax.random.fold_in(base_key, 2), M_WIN)
    waves = chosen[shuffle]
    jitter = jax.random.randint(jax.random.fold_in(base_key, 3), (M_WIN,), 0, 4)
    jitter = jnp.where(waves == 0, 0, jitter)
    headroom = NT - waves
    shorten = jnp.minimum(8 * jitter, headroom // 2)
    return (waves.astype(jnp.int32), (headroom - shorten).astype(jnp.int32))


def draw_wave_ids(key, part):
    return wave_table(key)[0]


def draw_trunc_lengths(key, part):
    return wave_table(key)[1]


def draw_cycle_points(key, part):
    cycle_index = jnp.arange(NHALF, dtype=jnp.int32)
    jitter = jax.random.randint(jax.random.fold_in(key, 21), (NHALF,), 0, 4)
    northern = jnp.minimum(LONMAX, 20 + 4 * cycle_index + 4 * jitter)
    return jnp.concatenate([northern, northern[::-1]]).astype(jnp.int32)


def levels(key, extent, shards, least, high):
    def one(dim, blocks):
        heights = jax.random.uniform(jax.random.fold_in(jax.random.fold_in(key, 6), dim), (blocks,), jnp.float32, least / len(shards), high / len(shards))
        return jnp.repeat(jnp.exp(heights), extent[dim] // blocks).reshape((-1,) + (1,) * (len(extent) - dim - 1))

    gain = one(*shards[0])
    for cut in shards[1:]:
        gain = gain * one(*cut)
    return gain


def noise(stream_key, dims, width, bound, split=(), kind=jnp.bfloat16):
    values = width * jax.random.normal(stream_key, dims, jnp.float32)
    if split:
        values = values * levels(stream_key, dims, split, -0.22, 0.18)
    return jnp.clip(values, -bound, bound).astype(kind)


def setup_inputs(seed: int = 0) -> dict:
    keys = jax.random.split(jax.random.key(seed), 11)
    spectral = noise(keys[0], (M_WIN, 2 * FIELDS, LEVELS, NT), 0.002, 0.01171875, ((0, 8), (2, 4)))
    legendre = noise(keys[1], (M_WIN, NHALF, NT), 1.0, 4.0, ((0, 8),))
    wave_ids = draw_wave_ids(jax.random.fold_in(keys[10], 71), 0)
    trunc_lengths = draw_trunc_lengths(jax.random.fold_in(keys[10], 71), 0)
    cycle_points = draw_cycle_points(jax.random.fold_in(keys[10], 71), 0)
    grid_coef = noise(keys[5], (NLAT, LONMAX), 1.0, 6.0, ((0, 8),), jnp.float32)
    cycle_weights = jnp.clip(jnp.exp(jax.random.uniform(keys[6], (NHALF,), jnp.float32, math.log(0.1), math.log(2.0))), 0.1, 2.0)
    modes_in = noise(keys[7], (LEVELS, LEVELS), LEVELS ** -0.5, 0.75)
    modes_out = noise(keys[8], (LEVELS, LEVELS), LEVELS ** -0.5, 0.75)
    depths = jnp.clip(jnp.exp(jax.random.uniform(keys[9], (LEVELS,), jnp.float32, math.log(0.05), math.log(20.0))), 0.05, 20.0)
    return {"spectral": spectral, "legendre": legendre, "wave_ids": wave_ids, "trunc_lengths": trunc_lengths, "cycle_points": cycle_points, "grid_coef": grid_coef, "cycle_weights": cycle_weights, "modes_in": modes_in, "modes_out": modes_out, "depths": depths}


def trig_rows(wave_ids, cycle_count, lon_max):
    longitude = jnp.arange(lon_max, dtype=jnp.int32)
    counts = cycle_count[:, None, None]
    phase_idx = (wave_ids[None, :, None] * longitude[None, None, :]) % counts
    angles = (2.0 * jnp.pi) * phase_idx.astype(jnp.float32) / counts.astype(jnp.float32)
    live_mask = (longitude[None, None, :] < counts) & (2 * wave_ids[None, :, None] < counts)
    cosine = jnp.where(live_mask, jnp.cos(angles), 0.0)
    sine_part = jnp.where(live_mask, -jnp.sin(angles), 0.0)
    return jnp.stack([cosine, sine_part], axis=1).astype(jnp.bfloat16)


def cycle_trip(fourier, wave_ids, cycle_count, coef_rows):
    wave_total, channels, items, group_size = fourier.shape
    fields = channels // 2
    polys = trig_rows(wave_ids, cycle_count, coef_rows.shape[1])
    factor = jnp.where(wave_ids == 0, 1.0, 2.0).astype(jnp.bfloat16)
    weighted = (fourier * factor[:, None, None, None]).reshape(wave_total, 2, fields, items, group_size)
    grid_vals = jnp.einsum("mrfig,grmk->gfik", weighted.astype(jnp.float32), polys.astype(jnp.float32))
    tendency = (grid_vals * (coef_rows[:, None, None, :] + jnp.roll(grid_vals, -1, axis=1))).astype(jnp.bfloat16)
    analysed = jnp.einsum("gfik,grmk->mrfig", tendency.astype(jnp.float32), polys.astype(jnp.float32))
    analysed = analysed / cycle_count.astype(jnp.float32)
    return analysed.astype(jnp.bfloat16).reshape(wave_total, channels, items, group_size)


def reference(spectral, legendre, wave_ids, trunc_lengths, cycle_points, grid_coef, cycle_weights, modes_in, modes_out, depths):
    wave_total, channels, levels_total, spec_len = spectral.shape
    half_lat = legendre.shape[1]
    lat_total = 2 * half_lat
    position = jnp.arange(spec_len, dtype=jnp.int32)
    parity_sign = jnp.where(position % 2 == 0, 1.0, -1.0).astype(jnp.bfloat16)

    def inverse_one(packed):
        coeffs, polys, length = packed
        flat = coeffs.reshape(-1, spec_len)
        flat = jnp.where(position[None, :] < length, flat, jnp.zeros_like(flat))
        northern = jnp.dot(flat, polys.T, preferred_element_type=jnp.float32)
        southern = jnp.dot(flat * parity_sign[None, :], polys.T, preferred_element_type=jnp.float32)
        joined = jnp.concatenate([northern, jnp.flip(southern, axis=1)], axis=1).astype(jnp.bfloat16)
        return joined.reshape(channels, levels_total, lat_total)

    fourier = lax.map(inverse_one, (spectral, legendre, trunc_lengths))

    group_size = math.gcd(lat_total, 32)
    groups = lat_total // group_size
    stacked = jnp.moveaxis(fourier.reshape(wave_total, channels, levels_total, groups, group_size), 3, 0)
    counts = cycle_points.reshape(groups, group_size)
    coefs = grid_coef.reshape(groups, group_size, -1)

    def group_trip(packed):
        return cycle_trip(packed[0], wave_ids, packed[1], packed[2])

    results = lax.map(group_trip, (stacked, counts, coefs))
    returned = jnp.moveaxis(results, 0, 3).reshape(wave_total, channels, levels_total, lat_total)

    def forward_one(packed):
        values, polys, length, wavenum = packed
        northern = values[..., :half_lat].astype(jnp.float32)
        southern = jnp.flip(values[..., half_lat:], axis=2).astype(jnp.float32)
        even_part = (cycle_weights * (northern + southern)).astype(jnp.bfloat16).reshape(-1, half_lat)
        odd_part = (cycle_weights * (northern - southern)).astype(jnp.bfloat16).reshape(-1, half_lat)
        from_even = jnp.dot(even_part, polys, preferred_element_type=jnp.float32)
        from_odd = jnp.dot(odd_part, polys, preferred_element_type=jnp.float32)
        coeffs = jnp.where(position[None, :] % 2 == 0, from_even, from_odd)
        coeffs = jnp.where(position[None, :] < length, coeffs, 0.0).astype(jnp.bfloat16)
        coeffs = coeffs.reshape(channels, levels_total, spec_len)
        mode_vals = jnp.einsum("kl,cli->cki", modes_in.astype(jnp.float32), coeffs.astype(jnp.float32))
        degree = (wavenum + position).astype(jnp.float32)
        damp = 1.0 / (1.0 + depths[:, None] * degree[None, :] * (degree[None, :] + 1.0) / float(NT * NT))
        scaled = (mode_vals * damp[None, :, :]).astype(jnp.bfloat16)
        mixed = jnp.einsum("lk,cki->cli", modes_out.astype(jnp.float32), scaled.astype(jnp.float32))
        return mixed.astype(jnp.bfloat16)

    return lax.map(forward_one, (returned, legendre, trunc_lengths, wave_ids))
```

```python
import functools

import jax
import jax.numpy as jnp
import numpy as np
from jax import lax
from jax.experimental import pallas as pl
from jax.experimental.pallas import tpu as pltpu
from jax.sharding import PartitionSpec as P

NT = 1280
LOW = 256
LANES = 128
NN = (((1,), (0,)), ((), ()))
NTD = (((1,), (1,)), ((), ()))
TN = (((0,), (0,)), ((), ()))
F32 = jnp.float32
BF16 = jnp.bfloat16


def turn_coefs(func, degree):
    nodes = 0.125 * (1.0 + np.cos(np.pi * (np.arange(degree + 1) + 0.5) / (degree + 1)))
    cheb = np.polynomial.Chebyshev.fit(nodes, func(nodes), degree, domain=[0.0, 0.25])
    return [float(v) for v in cheb.convert(kind=np.polynomial.Polynomial).coef]


COS = turn_coefs(lambda u: np.cos(2 * np.pi * np.sqrt(u)), 6)
SIN = turn_coefs(lambda u: np.sin(2 * np.pi * np.sqrt(u)) / np.sqrt(u), 6)


def horner(coefs, u):
    total = jnp.full_like(u, coefs[-1])
    for value in coefs[-2::-1]:
        total = total * u + value
    return total


def cos_sin(product, points, inverse):
    rest = product - jnp.round(product * inverse) * points
    turn = rest * inverse
    square = turn * turn
    return horner(COS, square), horner(SIN, square) * turn


def pad_to(value, unit):
    return -(-value // unit) * unit


def inverse_kernel(lengths, spec_ref, leg_ref, out_ref):
    shards, _, band, rows = out_ref.shape
    half = shards // 2
    length = lengths[pl.program_id(0)]
    _, channels, items, span = spec_ref.shape
    coeffs = spec_ref[0].reshape(rows, span)
    place = lax.broadcasted_iota(jnp.int32, (rows, span), 1)
    live = jnp.where(place < length, coeffs.astype(F32), 0.0)
    sign = jnp.where(place % 2 == 0, live, -live).astype(BF16)
    live = live.astype(BF16)
    wide = pad_to(rows, LANES)
    parts = [live, sign]
    if wide > rows:
        fill = jnp.zeros((wide - rows, span), BF16)
        parts = [live, fill, sign, fill]
    both = jnp.concatenate(parts, axis=0)
    for part in range(half):
        polys = leg_ref[0, part * band : (part + 1) * band, :]
        sums = lax.dot_general(polys, both, NTD, preferred_element_type=F32)
        out_ref[part, 0] = sums[:, :rows].astype(BF16)
        out_ref[shards - 1 - part, 0] = sums[:, wide : wide + rows].astype(BF16)


def inverse_legendre(spectral, legendre, lengths, shards):
    waves, channels, items, span = spectral.shape
    half_lat = legendre.shape[1]
    band = 2 * half_lat // shards
    rows = channels * items
    return pl.pallas_call(
        inverse_kernel,
        name="inverse",
        out_shape=jax.ShapeDtypeStruct((shards, waves, band, rows), BF16),
        grid_spec=pltpu.PrefetchScalarGridSpec(
            num_scalar_prefetch=1,
            grid=(waves,),
            in_specs=[
                pl.BlockSpec((1, channels, items, span), lambda m, s: (m, 0, 0, 0)),
                pl.BlockSpec((1, half_lat, span), lambda m, s: (m, 0, 0)),
            ],
            out_specs=pl.BlockSpec((shards, 1, band, rows), lambda m, s: (0, m, 0, 0)),
        ),
        compiler_params=pltpu.CompilerParams(vmem_limit_bytes=40 << 20),
        cost_estimate=pl.CostEstimate(
            flops=4 * waves * rows * half_lat * span,
            bytes_accessed=2 * waves * half_lat * span,
            transcendentals=0,
        ),
    )(lengths, spectral, legendre)


def forward_kernel(lengths, values_ref, leg_ref, weight_ref, out_ref):
    shards, _, band, rows = values_ref.shape
    half = shards // 2
    span = leg_ref.shape[2]
    length = lengths[pl.program_id(0)]
    north = jnp.concatenate([values_ref[k, 0] for k in range(half)], axis=0).astype(F32)
    south = jnp.concatenate(
        [values_ref[shards - 1 - k, 0] for k in range(half)], axis=0
    ).astype(F32)
    weights = weight_ref[:, :1]
    even = (weights * (north + south)).astype(BF16)
    odd = (weights * (north - south)).astype(BF16)
    polys = leg_ref[0]
    from_even = lax.dot_general(even, polys, TN, preferred_element_type=F32)
    from_odd = lax.dot_general(odd, polys, TN, preferred_element_type=F32)
    place = lax.broadcasted_iota(jnp.int32, (rows, span), 1)
    values = jnp.where(place % 2 == 0, from_even, from_odd)
    out_ref[0] = jnp.where(place < length, values, 0.0).astype(BF16)


def forward_legendre(returned, legendre, lengths, weights):
    shards, waves, band, rows = returned.shape
    half_lat, span = legendre.shape[1:]
    spread = jnp.broadcast_to(weights[:, None], (half_lat, LANES))
    return pl.pallas_call(
        forward_kernel,
        name="forward",
        out_shape=jax.ShapeDtypeStruct((waves, rows, span), BF16),
        grid_spec=pltpu.PrefetchScalarGridSpec(
            num_scalar_prefetch=1,
            grid=(waves,),
            in_specs=[
                pl.BlockSpec((shards, 1, band, rows), lambda m, s: (0, m, 0, 0)),
                pl.BlockSpec((1, half_lat, span), lambda m, s: (m, 0, 0)),
                pl.BlockSpec((half_lat, LANES), lambda m, s: (0, 0)),
            ],
            out_specs=pl.BlockSpec((1, rows, span), lambda m, s: (m, 0, 0)),
        ),
        compiler_params=pltpu.CompilerParams(vmem_limit_bytes=40 << 20),
        cost_estimate=pl.CostEstimate(
            flops=4 * waves * rows * half_lat * span,
            bytes_accessed=2 * waves * half_lat * span,
            transcendentals=0,
        ),
    )(lengths, returned, legendre, spread)


def cycle_kernel(
    fields, flip, points, inverses, in_ref, coef_ref, lane_ref, wave_ref, pick_ref, merge_ref, out_ref
):
    block, waves, both_rows = in_ref.shape
    rows = both_rows // 2
    items = rows // fields
    lon_max = coef_ref.shape[1]
    chunks = lon_max // LOW
    steps = pad_to(chunks, 8)
    wide = 4 * waves
    first = pl.program_id(0) * block
    reverse = flip[0]
    wave_lane = lane_ref[0:1, :]
    step_no = lax.broadcasted_iota(jnp.int32, (steps, wide), 0).astype(F32)
    step_wave = step_no * (wave_lane * float(LOW))
    low_no = lax.broadcasted_iota(jnp.int32, (waves, LOW), 1)
    low_wave = low_no.astype(F32) * wave_ref[...]
    wave_col = wave_ref[...]
    row_lane = lax.broadcasted_iota(jnp.int32, (waves, both_rows), 1)
    out_lane = lax.broadcasted_iota(jnp.int32, (rows, 2 * waves), 1)
    place = lax.broadcasted_iota(jnp.int32, (rows, LOW), 1).astype(F32)

    def one(local, carry):
        pts = points[first + local]
        inv = inverses[first + local]
        seat = local + reverse * (block - 1 - 2 * local)
        cos_step, sin_step = cos_sin(step_wave, pts, inv)
        synth = cos_step * lane_ref[1:2, :] + sin_step * lane_ref[2:3, :]
        anal = cos_step * lane_ref[3:4, :] + sin_step * lane_ref[4:5, :]
        cos_low, sin_low = cos_sin(low_wave, pts, inv)
        shown = 2.0 * wave_col < pts
        cos_low = jnp.where(shown, cos_low, 0.0).astype(BF16)
        sin_low = jnp.where(shown, -sin_low, 0.0).astype(BF16)
        table_in = jnp.concatenate([cos_low, sin_low, cos_low, sin_low], axis=0)
        table_out = jnp.concatenate([cos_low, sin_low, sin_low, cos_low], axis=0)

        data = in_ref[seat].astype(F32)
        real = jnp.where(row_lane < rows, data, 0.0).astype(BF16)
        imag = jnp.where(row_lane < rows, 0.0, data).astype(BF16)
        four = jnp.concatenate([real, imag, imag, real], axis=0)
        spread = lax.dot_general(pick_ref[...], four, NTD, preferred_element_type=F32)
        turned = jnp.concatenate(
            [(spread * synth[k : k + 1, :]).astype(BF16) for k in range(chunks)], axis=0
        )
        grid = lax.dot_general(turned, table_in, NN, preferred_element_type=F32)
        pieces = []
        for k in range(chunks):
            vals = grid[k * rows : (k + 1) * rows]
            after = jnp.concatenate([vals[items:], vals[:items]], axis=0)
            coef = coef_ref[pl.ds(local, 1), k * LOW : (k + 1) * LOW]
            tend = vals * (coef + after)
            pieces.append(jnp.where(place < pts - float(k * LOW), tend, 0.0).astype(BF16))
        tend = jnp.concatenate(pieces, axis=0)
        back = lax.dot_general(tend, table_out, NTD, preferred_element_type=F32)
        total = back[:rows] * anal[0:1, :]
        for k in range(1, chunks):
            total = total + back[k * rows : (k + 1) * rows] * anal[k : k + 1, :]
        result = (total[:, : 2 * waves] + total[:, 2 * waves :]) * inv
        split = jnp.concatenate(
            [
                jnp.where(out_lane < waves, result, 0.0).astype(BF16),
                jnp.where(out_lane < waves, 0.0, result).astype(BF16),
            ],
            axis=0,
        )
        out_ref[seat] = lax.dot_general(
            merge_ref[...], split, NTD, preferred_element_type=F32
        ).astype(BF16)
        return carry

    lax.fori_loop(0, block, one, 0, unroll=2)


def cycle_trips(values, wave_ids, points, coef, flip, fields):
    band, waves, both_rows = values.shape
    rows = both_rows // 2
    wide = 4 * waves
    lon_max = coef.shape[1]
    block = next(c for c in (40, 32, 16, 8) if band % c == 0)
    blocks = band // block
    lane = jnp.arange(wide)
    part = lane // waves
    wave_lane = jnp.tile(wave_ids, 4).astype(F32)
    factor = jnp.where(wave_lane == 0, 1.0, 2.0)
    own = (part < 2).astype(F32)
    cross = jnp.where(part == 2, -1.0, jnp.where(part == 3, 1.0, 0.0))
    zero = jnp.zeros_like(own)
    lanes = jnp.stack(
        [wave_lane, own * factor, cross * factor, own, -cross, zero, zero, zero], axis=0
    )
    wave_col = jnp.broadcast_to(wave_ids.astype(F32)[:, None], (waves, LOW))
    pick = (jnp.arange(rows)[:, None] == jnp.arange(both_rows)[None, :] % rows).astype(BF16)
    merge = (jnp.arange(waves)[:, None] == jnp.arange(2 * waves)[None, :] % waves).astype(BF16)

    def seat(b, s, *_):
        return (b + s[0] * (blocks - 1 - 2 * b), 0, 0)

    whole = lambda b, *_: (0, 0)
    return pl.pallas_call(
        functools.partial(cycle_kernel, fields),
        name="cycles",
        out_shape=jax.ShapeDtypeStruct((band, waves, both_rows), BF16),
        grid_spec=pltpu.PrefetchScalarGridSpec(
            num_scalar_prefetch=3,
            grid=(blocks,),
            in_specs=[
                pl.BlockSpec((block, waves, both_rows), seat),
                pl.BlockSpec((block, lon_max), lambda b, *_: (b, 0)),
                pl.BlockSpec((8, wide), whole),
                pl.BlockSpec((waves, LOW), whole),
                pl.BlockSpec((rows, both_rows), whole),
                pl.BlockSpec((waves, 2 * waves), whole),
            ],
            out_specs=pl.BlockSpec((block, waves, both_rows), seat),
        ),
        compiler_params=pltpu.CompilerParams(vmem_limit_bytes=40 << 20),
        cost_estimate=pl.CostEstimate(
            flops=8 * band * waves * rows * lon_max,
            bytes_accessed=4 * band * lon_max,
            transcendentals=0,
        ),
    )(
        flip,
        points.astype(F32),
        1.0 / points.astype(F32),
        values,
        coef,
        lanes,
        wave_col,
        pick,
        merge,
    )


def mode_kernel(channels, waves, all_ref, in_ref, out_ref_modes, depth_ref, ids, update_ref):
    shards, _, rows, span = all_ref.shape
    items = rows // channels
    wave = ids[pl.program_id(0)]
    modes = in_ref.shape[0]
    place = lax.broadcasted_iota(jnp.int32, (modes, span), 1)
    degree = (place + wave).astype(F32)
    damp = 1.0 / (1.0 + depth_ref[:, :1] * degree * (degree + 1.0) / float(NT * NT))
    for c in range(channels):
        stack = jnp.concatenate(
            [all_ref[s, 0, c * items : (c + 1) * items, :] for s in range(shards)], axis=0
        )
        vals = lax.dot_general(in_ref[...], stack, NN, preferred_element_type=F32)
        scaled = (vals * damp).astype(BF16)
        update_ref[0, c] = lax.dot_general(
            out_ref_modes[...], scaled, NN, preferred_element_type=F32
        ).astype(BF16)


def vertical(gathered, modes_in, own_rows, depths, own_waves, channels):
    shards, waves, rows, span = gathered.shape
    items = rows // channels
    modes, levels = modes_in.shape
    spread = jnp.broadcast_to(depths[:, None], (modes, LANES))

    def body(ids, all_ref, in_ref, own_ref, depth_ref, update_ref):
        mode_kernel(channels, waves, all_ref, in_ref, own_ref, depth_ref, ids, update_ref)

    return pl.pallas_call(
        body,
        name="vertical",
        out_shape=jax.ShapeDtypeStruct((waves, channels, items, span), BF16),
        grid_spec=pltpu.PrefetchScalarGridSpec(
            num_scalar_prefetch=1,
            grid=(waves,),
            in_specs=[
                pl.BlockSpec((shards, 1, rows, span), lambda m, s: (0, m, 0, 0)),
                pl.BlockSpec((modes, levels), lambda m, s: (0, 0)),
                pl.BlockSpec((items, modes), lambda m, s: (0, 0)),
                pl.BlockSpec((modes, LANES), lambda m, s: (0, 0)),
            ],
            out_specs=pl.BlockSpec((1, channels, items, span), lambda m, s: (m, 0, 0, 0)),
        ),
        compiler_params=pltpu.CompilerParams(vmem_limit_bytes=40 << 20),
    )(own_waves, gathered, modes_in, own_rows, spread)


def on_device(
    spectral,
    legendre,
    wave_ids,
    trunc_lengths,
    cycle_points,
    grid_coef,
    cycle_weights,
    modes_in,
    modes_out,
    depths,
):
    wave_rank = lax.axis_index("wave")
    lev_rank = lax.axis_index("lev")
    shards = lax.axis_size("wave")
    waves, channels, items, span = spectral.shape
    rows = channels * items
    band = grid_coef.shape[0]
    own_waves = lax.dynamic_slice_in_dim(wave_ids, wave_rank * waves, waves)
    own_lengths = lax.dynamic_slice_in_dim(trunc_lengths, wave_rank * waves, waves)
    fourier = inverse_legendre(spectral, legendre, own_lengths, shards)
    arrived = lax.all_to_all(fourier, "wave", split_axis=0, concat_axis=0, tiled=True)
    by_cycle = jnp.swapaxes(arrived.reshape(shards * waves, band, rows), 0, 1)
    points = lax.dynamic_slice_in_dim(cycle_points, wave_rank * band, band)
    flip = (wave_rank >= shards // 2).astype(jnp.int32).reshape(1)
    analysed = cycle_trips(by_cycle, wave_ids, points, grid_coef, flip, channels // 2)
    leaving = jnp.swapaxes(analysed, 0, 1).reshape(shards, waves, band, rows)
    returned = lax.all_to_all(leaving, "wave", split_axis=0, concat_axis=0, tiled=True)
    projected = forward_legendre(returned, legendre, own_lengths, cycle_weights)
    gathered = lax.all_gather(projected, "lev", axis=0)
    own_rows = lax.dynamic_slice_in_dim(modes_out, lev_rank * items, items, 0)
    return vertical(gathered, modes_in, own_rows, depths, own_waves, channels)


def solution(mesh):
    placed = (
        P("wave", None, "lev", None),
        P("wave", None, None),
        P(),
        P(),
        P(),
        P("wave", None),
        P(),
        P(),
        P(),
        P(),
    )
    return jax.shard_map(
        on_device,
        mesh=mesh,
        in_specs=placed,
        out_specs=P("wave", None, "lev", None),
        check_vma=False,
    )
```

```python
import functools

import jax
import jax.numpy as jnp
import numpy as np
from jax import lax
from jax.experimental import pallas as pl
from jax.experimental.pallas import tpu as pltpu
from jax.sharding import PartitionSpec as P

NT = 1280
LOW = 256
LANES = 128
GROUP = 4
NN = (((1,), (0,)), ((), ()))
NTD = (((1,), (1,)), ((), ()))
TN = (((0,), (0,)), ((), ()))
F32 = jnp.float32
BF16 = jnp.bfloat16


def turn_coefs(func, degree):
    nodes = 0.125 * (1.0 + np.cos(np.pi * (np.arange(degree + 1) + 0.5) / (degree + 1)))
    cheb = np.polynomial.Chebyshev.fit(nodes, func(nodes), degree, domain=[0.0, 0.25])
    return [float(v) for v in cheb.convert(kind=np.polynomial.Polynomial).coef]


COS = turn_coefs(lambda u: np.cos(2 * np.pi * np.sqrt(u)), 6)
SIN = turn_coefs(lambda u: np.sin(2 * np.pi * np.sqrt(u)) / np.sqrt(u), 6)


def horner(coefs, u):
    total = jnp.full_like(u, coefs[-1])
    for value in coefs[-2::-1]:
        total = total * u + value
    return total


def cos_sin(product, points, inverse):
    rest = product - jnp.round(product * inverse) * points
    turn = rest * inverse
    square = turn * turn
    return horner(COS, square), horner(SIN, square) * turn


def pad_to(value, unit):
    return -(-value // unit) * unit


def inverse_kernel(lengths, spec_ref, leg_ref, out_ref):
    shards, _, band, rows = out_ref.shape
    half = shards // 2
    length = lengths[pl.program_id(0)]
    _, channels, items, span = spec_ref.shape
    coeffs = spec_ref[0].reshape(rows, span)
    place = lax.broadcasted_iota(jnp.int32, (rows, span), 1)
    live = jnp.where(place < length, coeffs.astype(F32), 0.0)
    sign = jnp.where(place % 2 == 0, live, -live).astype(BF16)
    live = live.astype(BF16)
    wide = pad_to(rows, LANES)
    parts = [live, sign]
    if wide > rows:
        fill = jnp.zeros((wide - rows, span), BF16)
        parts = [live, fill, sign, fill]
    both = jnp.concatenate(parts, axis=0)
    for part in range(half):
        polys = leg_ref[0, part * band : (part + 1) * band, :]
        sums = lax.dot_general(polys, both, NTD, preferred_element_type=F32)
        out_ref[part, 0] = sums[:, :rows].astype(BF16)
        out_ref[shards - 1 - part, 0] = sums[:, wide : wide + rows].astype(BF16)


def inverse_legendre(spectral, legendre, lengths, shards):
    waves, channels, items, span = spectral.shape
    half_lat = legendre.shape[1]
    band = 2 * half_lat // shards
    rows = channels * items
    return pl.pallas_call(
        inverse_kernel,
        name="inverse",
        out_shape=jax.ShapeDtypeStruct((shards, waves, band, rows), BF16),
        grid_spec=pltpu.PrefetchScalarGridSpec(
            num_scalar_prefetch=1,
            grid=(waves,),
            in_specs=[
                pl.BlockSpec((1, channels, items, span), lambda m, s: (m, 0, 0, 0)),
                pl.BlockSpec((1, half_lat, span), lambda m, s: (m, 0, 0)),
            ],
            out_specs=pl.BlockSpec((shards, 1, band, rows), lambda m, s: (0, m, 0, 0)),
        ),
        compiler_params=pltpu.CompilerParams(vmem_limit_bytes=40 << 20),
        cost_estimate=pl.CostEstimate(
            flops=4 * waves * rows * half_lat * span,
            bytes_accessed=2 * waves * half_lat * span,
            transcendentals=0,
        ),
    )(lengths, spectral, legendre)


def forward_kernel(lengths, values_ref, leg_ref, weight_ref, out_ref):
    shards, _, band, rows = values_ref.shape
    half = shards // 2
    span = leg_ref.shape[2]
    length = lengths[pl.program_id(0)]
    north = jnp.concatenate([values_ref[k, 0] for k in range(half)], axis=0).astype(F32)
    south = jnp.concatenate(
        [values_ref[shards - 1 - k, 0] for k in range(half)], axis=0
    ).astype(F32)
    weights = weight_ref[:, :1]
    even = (weights * (north + south)).astype(BF16)
    odd = (weights * (north - south)).astype(BF16)
    polys = leg_ref[0]
    from_even = lax.dot_general(even, polys, TN, preferred_element_type=F32)
    from_odd = lax.dot_general(odd, polys, TN, preferred_element_type=F32)
    place = lax.broadcasted_iota(jnp.int32, (rows, span), 1)
    values = jnp.where(place % 2 == 0, from_even, from_odd)
    out_ref[0] = jnp.where(place < length, values, 0.0).astype(BF16)


def forward_legendre(returned, legendre, lengths, weights):
    shards, waves, band, rows = returned.shape
    half_lat, span = legendre.shape[1:]
    spread = jnp.broadcast_to(weights[:, None], (half_lat, LANES))
    return pl.pallas_call(
        forward_kernel,
        name="forward",
        out_shape=jax.ShapeDtypeStruct((waves, rows, span), BF16),
        grid_spec=pltpu.PrefetchScalarGridSpec(
            num_scalar_prefetch=1,
            grid=(waves,),
            in_specs=[
                pl.BlockSpec((shards, 1, band, rows), lambda m, s: (0, m, 0, 0)),
                pl.BlockSpec((1, half_lat, span), lambda m, s: (m, 0, 0)),
                pl.BlockSpec((half_lat, LANES), lambda m, s: (0, 0)),
            ],
            out_specs=pl.BlockSpec((1, rows, span), lambda m, s: (m, 0, 0)),
        ),
        compiler_params=pltpu.CompilerParams(vmem_limit_bytes=40 << 20),
        cost_estimate=pl.CostEstimate(
            flops=4 * waves * rows * half_lat * span,
            bytes_accessed=2 * waves * half_lat * span,
            transcendentals=0,
        ),
    )(lengths, returned, legendre, spread)


def cycle_kernel(
    fields, flip, points, inverses, in_ref, coef_ref, lane_ref, wave_ref, pick_ref, merge_ref, out_ref
):
    block, waves, both_rows = in_ref.shape
    rows = both_rows // 2
    items = rows // fields
    lon_max = coef_ref.shape[1]
    chunks = lon_max // LOW
    steps = pad_to(chunks, 8)
    wide = 4 * waves
    first = pl.program_id(0) * block
    reverse = flip[0]
    wave_lane = lane_ref[0:1, :]
    step_no = lax.broadcasted_iota(jnp.int32, (steps, wide), 0).astype(F32)
    step_wave = step_no * (wave_lane * float(LOW))
    low_no = lax.broadcasted_iota(jnp.int32, (waves, LOW), 1)
    low_wave = low_no.astype(F32) * wave_ref[...]
    wave_col = wave_ref[...]
    row_lane = lax.broadcasted_iota(jnp.int32, (waves, both_rows), 1)
    out_lane = lax.broadcasted_iota(jnp.int32, (rows, 2 * waves), 1)
    place = lax.broadcasted_iota(jnp.int32, (rows, LOW), 1).astype(F32)

    def prepare(local):
        pts = points[first + local]
        inv = inverses[first + local]
        cos_step, sin_step = cos_sin(step_wave, pts, inv)
        synth = cos_step * lane_ref[1:2, :] + sin_step * lane_ref[2:3, :]
        anal = cos_step * lane_ref[3:4, :] + sin_step * lane_ref[4:5, :]
        cos_low, sin_low = cos_sin(low_wave, pts, inv)
        shown = 2.0 * wave_col < pts
        cos_low = jnp.where(shown, cos_low, 0.0).astype(BF16)
        sin_low = jnp.where(shown, -sin_low, 0.0).astype(BF16)
        return pts, inv, synth, anal, cos_low, sin_low

    def pick(seat):
        data = in_ref[seat].astype(F32)
        real = jnp.where(row_lane < rows, data, 0.0).astype(BF16)
        imag = jnp.where(row_lane < rows, 0.0, data).astype(BF16)
        four = jnp.concatenate([real, imag, imag, real], axis=0)
        return lax.dot_general(pick_ref[...], four, NTD, preferred_element_type=F32)

    def tendency(grid, local, pts):
        pieces = []
        for k in range(chunks):
            vals = grid[k * rows : (k + 1) * rows]
            after = jnp.concatenate([vals[items:], vals[:items]], axis=0)
            coef = coef_ref[pl.ds(local, 1), k * LOW : (k + 1) * LOW]
            tend = vals * (coef + after)
            pieces.append(jnp.where(place < pts - float(k * LOW), tend, 0.0).astype(BF16))
        return jnp.concatenate(pieces, axis=0)

    def reduce(back, anal, inv):
        total = back[:rows] * anal[0:1, :]
        for k in range(1, chunks):
            total = total + back[k * rows : (k + 1) * rows] * anal[k : k + 1, :]
        result = (total[:, : 2 * waves] + total[:, 2 * waves :]) * inv
        return jnp.concatenate(
            [
                jnp.where(out_lane < waves, result, 0.0).astype(BF16),
                jnp.where(out_lane < waves, 0.0, result).astype(BF16),
            ],
            axis=0,
        )

    def several(step, carry):
        locals_ = [step * GROUP + g for g in range(GROUP)]
        seats = [v + reverse * (block - 1 - 2 * v) for v in locals_]
        made = [prepare(v) for v in locals_]
        spreads = [pick(v) for v in seats]
        turned = [
            jnp.concatenate(
                [(x * w[2][k : k + 1, :]).astype(BF16) for k in range(chunks)], axis=0
            )
            for x, w in zip(spreads, made)
        ]
        grids = [
            lax.dot_general(
                x,
                jnp.concatenate([w[4], w[5], w[4], w[5]], axis=0),
                NN,
                preferred_element_type=F32,
            )
            for x, w in zip(turned, made)
        ]
        tends = [tendency(x, v, w[0]) for x, v, w in zip(grids, locals_, made)]
        backs = [
            lax.dot_general(
                x,
                jnp.concatenate([w[4], w[5], w[5], w[4]], axis=0),
                NTD,
                preferred_element_type=F32,
            )
            for x, w in zip(tends, made)
        ]
        splits = [reduce(x, w[3], w[1]) for x, w in zip(backs, made)]
        outs = [
            lax.dot_general(merge_ref[...], x, NTD, preferred_element_type=F32).astype(BF16)
            for x in splits
        ]
        for seat, value in zip(seats, outs):
            out_ref[seat] = value
        return carry

    lax.fori_loop(0, block // GROUP, several, 0)


def cycle_trips(values, wave_ids, points, coef, flip, fields):
    band, waves, both_rows = values.shape
    rows = both_rows // 2
    wide = 4 * waves
    lon_max = coef.shape[1]
    block = next(c for c in (40, 32, 16, 8) if band % c == 0)
    blocks = band // block
    lane = jnp.arange(wide)
    part = lane // waves
    wave_lane = jnp.tile(wave_ids, 4).astype(F32)
    factor = jnp.where(wave_lane == 0, 1.0, 2.0)
    own = (part < 2).astype(F32)
    cross = jnp.where(part == 2, -1.0, jnp.where(part == 3, 1.0, 0.0))
    zero = jnp.zeros_like(own)
    lanes = jnp.stack(
        [wave_lane, own * factor, cross * factor, own, -cross, zero, zero, zero], axis=0
    )
    wave_col = jnp.broadcast_to(wave_ids.astype(F32)[:, None], (waves, LOW))
    pick = (jnp.arange(rows)[:, None] == jnp.arange(both_rows)[None, :] % rows).astype(BF16)
    merge = (jnp.arange(waves)[:, None] == jnp.arange(2 * waves)[None, :] % waves).astype(BF16)

    def seat(b, s, *_):
        return (b + s[0] * (blocks - 1 - 2 * b), 0, 0)

    whole = lambda b, *_: (0, 0)
    return pl.pallas_call(
        functools.partial(cycle_kernel, fields),
        name="cycles",
        out_shape=jax.ShapeDtypeStruct((band, waves, both_rows), BF16),
        grid_spec=pltpu.PrefetchScalarGridSpec(
            num_scalar_prefetch=3,
            grid=(blocks,),
            in_specs=[
                pl.BlockSpec((block, waves, both_rows), seat),
                pl.BlockSpec((block, lon_max), lambda b, *_: (b, 0)),
                pl.BlockSpec((8, wide), whole),
                pl.BlockSpec((waves, LOW), whole),
                pl.BlockSpec((rows, both_rows), whole),
                pl.BlockSpec((waves, 2 * waves), whole),
            ],
            out_specs=pl.BlockSpec((block, waves, both_rows), seat),
        ),
        compiler_params=pltpu.CompilerParams(vmem_limit_bytes=40 << 20),
        cost_estimate=pl.CostEstimate(
            flops=8 * band * waves * rows * lon_max,
            bytes_accessed=4 * band * lon_max,
            transcendentals=0,
        ),
    )(
        flip,
        points.astype(F32),
        1.0 / points.astype(F32),
        values,
        coef,
        lanes,
        wave_col,
        pick,
        merge,
    )


def mode_kernel(channels, waves, all_ref, in_ref, out_ref_modes, depth_ref, ids, update_ref):
    shards, _, rows, span = all_ref.shape
    items = rows // channels
    wave = ids[pl.program_id(0)]
    modes = in_ref.shape[0]
    place = lax.broadcasted_iota(jnp.int32, (modes, span), 1)
    degree = (place + wave).astype(F32)
    damp = 1.0 / (1.0 + depth_ref[:, :1] * degree * (degree + 1.0) / float(NT * NT))
    for c in range(channels):
        stack = jnp.concatenate(
            [all_ref[s, 0, c * items : (c + 1) * items, :] for s in range(shards)], axis=0
        )
        vals = lax.dot_general(in_ref[...], stack, NN, preferred_element_type=F32)
        scaled = (vals * damp).astype(BF16)
        update_ref[0, c] = lax.dot_general(
            out_ref_modes[...], scaled, NN, preferred_element_type=F32
        ).astype(BF16)


def vertical(gathered, modes_in, own_rows, depths, own_waves, channels):
    shards, waves, rows, span = gathered.shape
    items = rows // channels
    modes, levels = modes_in.shape
    spread = jnp.broadcast_to(depths[:, None], (modes, LANES))

    def body(ids, all_ref, in_ref, own_ref, depth_ref, update_ref):
        mode_kernel(channels, waves, all_ref, in_ref, own_ref, depth_ref, ids, update_ref)

    return pl.pallas_call(
        body,
        name="vertical",
        out_shape=jax.ShapeDtypeStruct((waves, channels, items, span), BF16),
        grid_spec=pltpu.PrefetchScalarGridSpec(
            num_scalar_prefetch=1,
            grid=(waves,),
            in_specs=[
                pl.BlockSpec((shards, 1, rows, span), lambda m, s: (0, m, 0, 0)),
                pl.BlockSpec((modes, levels), lambda m, s: (0, 0)),
                pl.BlockSpec((items, modes), lambda m, s: (0, 0)),
                pl.BlockSpec((modes, LANES), lambda m, s: (0, 0)),
            ],
            out_specs=pl.BlockSpec((1, channels, items, span), lambda m, s: (m, 0, 0, 0)),
        ),
        compiler_params=pltpu.CompilerParams(vmem_limit_bytes=40 << 20),
    )(own_waves, gathered, modes_in, own_rows, spread)


def on_device(
    spectral,
    legendre,
    wave_ids,
    trunc_lengths,
    cycle_points,
    grid_coef,
    cycle_weights,
    modes_in,
    modes_out,
    depths,
):
    wave_rank = lax.axis_index("wave")
    lev_rank = lax.axis_index("lev")
    shards = lax.axis_size("wave")
    waves, channels, items, span = spectral.shape
    rows = channels * items
    band = grid_coef.shape[0]
    own_waves = lax.dynamic_slice_in_dim(wave_ids, wave_rank * waves, waves)
    own_lengths = lax.dynamic_slice_in_dim(trunc_lengths, wave_rank * waves, waves)
    fourier = inverse_legendre(spectral, legendre, own_lengths, shards)
    arrived = lax.all_to_all(fourier, "wave", split_axis=0, concat_axis=0, tiled=True)
    by_cycle = jnp.swapaxes(arrived.reshape(shards * waves, band, rows), 0, 1)
    points = lax.dynamic_slice_in_dim(cycle_points, wave_rank * band, band)
    flip = (wave_rank >= shards // 2).astype(jnp.int32).reshape(1)
    analysed = cycle_trips(by_cycle, wave_ids, points, grid_coef, flip, channels // 2)
    leaving = jnp.swapaxes(analysed, 0, 1).reshape(shards, waves, band, rows)
    returned = lax.all_to_all(leaving, "wave", split_axis=0, concat_axis=0, tiled=True)
    projected = forward_legendre(returned, legendre, own_lengths, cycle_weights)
    gathered = lax.all_gather(projected, "lev", axis=0)
    own_rows = lax.dynamic_slice_in_dim(modes_out, lev_rank * items, items, 0)
    return vertical(gathered, modes_in, own_rows, depths, own_waves, channels)


def solution(mesh):
    placed = (
        P("wave", None, "lev", None),
        P("wave", None, None),
        P(),
        P(),
        P(),
        P("wave", None),
        P(),
        P(),
        P(),
        P(),
    )
    return jax.shard_map(
        on_device,
        mesh=mesh,
        in_specs=placed,
        out_specs=P("wave", None, "lev", None),
        check_vma=False,
    )
```

```python
import functools

import jax
import jax.numpy as jnp
import numpy as np
from jax import lax
from jax.experimental import pallas as pl
from jax.experimental.pallas import tpu as pltpu
from jax.sharding import PartitionSpec as P

NT = 1280
LOW = 256
LANES = 128
GROUP = 4
NN = (((1,), (0,)), ((), ()))
NTD = (((1,), (1,)), ((), ()))
TN = (((0,), (0,)), ((), ()))
F32 = jnp.float32
BF16 = jnp.bfloat16


def turn_coefs(func, degree):
    nodes = 0.125 * (1.0 + np.cos(np.pi * (np.arange(degree + 1) + 0.5) / (degree + 1)))
    cheb = np.polynomial.Chebyshev.fit(nodes, func(nodes), degree, domain=[0.0, 0.25])
    return [float(v) for v in cheb.convert(kind=np.polynomial.Polynomial).coef]


COS = turn_coefs(lambda u: np.cos(2 * np.pi * np.sqrt(u)), 6)
SIN = turn_coefs(lambda u: np.sin(2 * np.pi * np.sqrt(u)) / np.sqrt(u), 6)


def horner(coefs, u):
    total = jnp.full_like(u, coefs[-1])
    for value in coefs[-2::-1]:
        total = total * u + value
    return total


def cos_sin(product, points, inverse):
    rest = product - jnp.round(product * inverse) * points
    turn = rest * inverse
    square = turn * turn
    return horner(COS, square), horner(SIN, square) * turn


def pad_to(value, unit):
    return -(-value // unit) * unit


def inverse_kernel(lengths, spec_ref, leg_ref, out_ref):
    shards, _, band, rows = out_ref.shape
    half = shards // 2
    length = lengths[pl.program_id(0)]
    _, channels, items, span = spec_ref.shape
    coeffs = spec_ref[0].reshape(rows, span)
    place = lax.broadcasted_iota(jnp.int32, (rows, span), 1)
    live = jnp.where(place < length, coeffs.astype(F32), 0.0)
    sign = jnp.where(place % 2 == 0, live, -live).astype(BF16)
    live = live.astype(BF16)
    wide = pad_to(rows, LANES)
    parts = [live, sign]
    if wide > rows:
        fill = jnp.zeros((wide - rows, span), BF16)
        parts = [live, fill, sign, fill]
    both = jnp.concatenate(parts, axis=0)
    for part in range(half):
        polys = leg_ref[0, part * band : (part + 1) * band, :]
        sums = lax.dot_general(polys, both, NTD, preferred_element_type=F32)
        out_ref[part, 0] = sums[:, :rows].astype(BF16)
        out_ref[shards - 1 - part, 0] = sums[:, wide : wide + rows].astype(BF16)


def inverse_legendre(spectral, legendre, lengths, shards):
    waves, channels, items, span = spectral.shape
    half_lat = legendre.shape[1]
    band = 2 * half_lat // shards
    rows = channels * items
    return pl.pallas_call(
        inverse_kernel,
        name="inverse",
        out_shape=jax.ShapeDtypeStruct((shards, waves, band, rows), BF16),
        grid_spec=pltpu.PrefetchScalarGridSpec(
            num_scalar_prefetch=1,
            grid=(waves,),
            in_specs=[
                pl.BlockSpec((1, channels, items, span), lambda m, s: (m, 0, 0, 0)),
                pl.BlockSpec((1, half_lat, span), lambda m, s: (m, 0, 0)),
            ],
            out_specs=pl.BlockSpec((shards, 1, band, rows), lambda m, s: (0, m, 0, 0)),
        ),
        compiler_params=pltpu.CompilerParams(vmem_limit_bytes=40 << 20),
        cost_estimate=pl.CostEstimate(
            flops=4 * waves * rows * half_lat * span,
            bytes_accessed=2 * waves * half_lat * span,
            transcendentals=0,
        ),
    )(lengths, spectral, legendre)


def forward_kernel(lengths, values_ref, leg_ref, weight_ref, out_ref):
    shards, _, band, rows = values_ref.shape
    half = shards // 2
    span = leg_ref.shape[2]
    length = lengths[pl.program_id(0)]
    north = jnp.concatenate([values_ref[k, 0] for k in range(half)], axis=0).astype(F32)
    south = jnp.concatenate(
        [values_ref[shards - 1 - k, 0] for k in range(half)], axis=0
    ).astype(F32)
    weights = weight_ref[:, :1]
    even = (weights * (north + south)).astype(BF16)
    odd = (weights * (north - south)).astype(BF16)
    polys = leg_ref[0]
    from_even = lax.dot_general(even, polys, TN, preferred_element_type=F32)
    from_odd = lax.dot_general(odd, polys, TN, preferred_element_type=F32)
    place = lax.broadcasted_iota(jnp.int32, (rows, span), 1)
    values = jnp.where(place % 2 == 0, from_even, from_odd)
    out_ref[0] = jnp.where(place < length, values, 0.0).astype(BF16)


def forward_legendre(returned, legendre, lengths, weights):
    shards, waves, band, rows = returned.shape
    half_lat, span = legendre.shape[1:]
    spread = jnp.broadcast_to(weights[:, None], (half_lat, LANES))
    return pl.pallas_call(
        forward_kernel,
        name="forward",
        out_shape=jax.ShapeDtypeStruct((waves, rows, span), BF16),
        grid_spec=pltpu.PrefetchScalarGridSpec(
            num_scalar_prefetch=1,
            grid=(waves,),
            in_specs=[
                pl.BlockSpec((shards, 1, band, rows), lambda m, s: (0, m, 0, 0)),
                pl.BlockSpec((1, half_lat, span), lambda m, s: (m, 0, 0)),
                pl.BlockSpec((half_lat, LANES), lambda m, s: (0, 0)),
            ],
            out_specs=pl.BlockSpec((1, rows, span), lambda m, s: (m, 0, 0)),
        ),
        compiler_params=pltpu.CompilerParams(vmem_limit_bytes=40 << 20),
        cost_estimate=pl.CostEstimate(
            flops=4 * waves * rows * half_lat * span,
            bytes_accessed=2 * waves * half_lat * span,
            transcendentals=0,
        ),
    )(lengths, returned, legendre, spread)


def exchange_kernel(
    fields,
    chunk,
    points,
    inverses,
    sent_ref,
    coef_ref,
    lane_ref,
    wave_ref,
    pick_ref,
    merge_ref,
    back_ref,
    land_ref,
    leave_ref,
    in_ref,
    out_ref,
    in_send,
    in_recv,
    out_send,
    out_recv,
    own_sems,
):
    shards, local_waves, band, both_rows = sent_ref.shape
    waves = shards * local_waves
    rows = both_rows // 2
    items = rows // fields
    lon_max = coef_ref.shape[1]
    chunks = lon_max // LOW
    steps = pad_to(chunks, 8)
    wide = 4 * waves
    me = lax.axis_index("wave")
    reverse = (me * 2) // shards

    barrier = pltpu.get_barrier_semaphore()
    for away in range(1, shards):
        pl.semaphore_signal(
            barrier,
            inc=1,
            device_id={"wave": lax.rem(me + away, shards)},
            device_id_type=pl.DeviceIdType.MESH,
        )
    pl.semaphore_wait(barrier, shards - 1)

    def span_of(part):
        return pl.ds(pl.multiple_of(part * chunk, chunk), chunk)

    def remote(src, dst, send, recv, away, part):
        to = lax.rem(me + away, shards)
        return pltpu.make_async_remote_copy(
            src_ref=src.at[to, :, span_of(part), :],
            dst_ref=dst.at[me, :, span_of(part), :],
            send_sem=send.at[away - 1, part],
            recv_sem=recv.at[away - 1, part],
            device_id={"wave": to},
            device_id_type=pl.DeviceIdType.MESH,
        )

    def own(src, dst, which, part):
        return pltpu.make_async_copy(
            src.at[me, :, span_of(part), :],
            dst.at[me, :, span_of(part), :],
            own_sems.at[which, part],
        )

    def start_in(part, carry):
        for away in range(1, shards):
            remote(sent_ref, land_ref, in_send, in_recv, away, part).start()
        own(sent_ref, land_ref, 0, part).start()
        return carry

    lax.fori_loop(0, band // chunk, start_in, 0)

    wave_lane = lane_ref[0:1, :]
    step_no = lax.broadcasted_iota(jnp.int32, (steps, wide), 0).astype(F32)
    step_wave = step_no * (wave_lane * float(LOW))
    low_no = lax.broadcasted_iota(jnp.int32, (waves, LOW), 1)
    low_wave = low_no.astype(F32) * wave_ref[...]
    wave_col = wave_ref[...]
    row_lane = lax.broadcasted_iota(jnp.int32, (waves, both_rows), 1)
    out_lane = lax.broadcasted_iota(jnp.int32, (rows, 2 * waves), 1)
    place = lax.broadcasted_iota(jnp.int32, (rows, LOW), 1).astype(F32)

    def prepare(local):
        pts = points[local]
        inv = inverses[local]
        cos_step, sin_step = cos_sin(step_wave, pts, inv)
        synth = cos_step * lane_ref[1:2, :] + sin_step * lane_ref[2:3, :]
        anal = cos_step * lane_ref[3:4, :] + sin_step * lane_ref[4:5, :]
        cos_low, sin_low = cos_sin(low_wave, pts, inv)
        shown = 2.0 * wave_col < pts
        cos_low = jnp.where(shown, cos_low, 0.0).astype(BF16)
        sin_low = jnp.where(shown, -sin_low, 0.0).astype(BF16)
        return pts, inv, synth, anal, cos_low, sin_low

    def pick(seat):
        data = in_ref[seat]
        real = jnp.where(row_lane < rows, data, 0.0).astype(BF16)
        imag = jnp.where(row_lane < rows, 0.0, data).astype(BF16)
        four = jnp.concatenate([real, imag, imag, real], axis=0)
        return lax.dot_general(pick_ref[...], four, NTD, preferred_element_type=F32)

    def tendency(grid, local, pts):
        pieces = []
        for k in range(chunks):
            vals = grid[k * rows : (k + 1) * rows]
            after = jnp.concatenate([vals[items:], vals[:items]], axis=0)
            coef = coef_ref[pl.ds(local, 1), k * LOW : (k + 1) * LOW]
            tend = vals * (coef + after)
            pieces.append(jnp.where(place < pts - float(k * LOW), tend, 0.0).astype(BF16))
        return jnp.concatenate(pieces, axis=0)

    def reduce(back, anal, inv):
        total = back[:rows] * anal[0:1, :]
        for k in range(1, chunks):
            total = total + back[k * rows : (k + 1) * rows] * anal[k : k + 1, :]
        result = (total[:, : 2 * waves] + total[:, 2 * waves :]) * inv
        return jnp.concatenate(
            [
                jnp.where(out_lane < waves, result, 0.0).astype(BF16),
                jnp.where(out_lane < waves, 0.0, result).astype(BF16),
            ],
            axis=0,
        )

    def several(part, step, carry):
        seats = [step * GROUP + g for g in range(GROUP)]
        stored = [part * chunk + v for v in seats]
        locals_ = [v + reverse * (band - 1 - 2 * v) for v in stored]
        made = [prepare(v) for v in locals_]
        spreads = [pick(v) for v in seats]
        turned = [
            jnp.concatenate(
                [(x * w[2][k : k + 1, :]).astype(BF16) for k in range(chunks)], axis=0
            )
            for x, w in zip(spreads, made)
        ]
        grids = [
            lax.dot_general(
                x,
                jnp.concatenate([w[4], w[5], w[4], w[5]], axis=0),
                NN,
                preferred_element_type=F32,
            )
            for x, w in zip(turned, made)
        ]
        tends = [tendency(x, v, w[0]) for x, v, w in zip(grids, locals_, made)]
        backs = [
            lax.dot_general(
                x,
                jnp.concatenate([w[4], w[5], w[5], w[4]], axis=0),
                NTD,
                preferred_element_type=F32,
            )
            for x, w in zip(tends, made)
        ]
        splits = [reduce(x, w[3], w[1]) for x, w in zip(backs, made)]
        outs = [
            lax.dot_general(merge_ref[...], x, NTD, preferred_element_type=F32)
            for x in splits
        ]
        for seat, value in zip(seats, outs):
            out_ref[seat] = value
        return carry

    def work(part, carry):
        for away in range(1, shards):
            remote(sent_ref, land_ref, in_send, in_recv, away, part).wait_recv()
        own(sent_ref, land_ref, 0, part).wait()
        got = land_ref[:, :, span_of(part), :].reshape(waves, chunk, both_rows)
        in_ref[...] = jnp.swapaxes(got.astype(F32), 0, 1)
        lax.fori_loop(0, chunk // GROUP, functools.partial(several, part), 0)
        made = jnp.swapaxes(out_ref[...], 0, 1).astype(BF16)
        leave_ref[:, :, span_of(part), :] = made.reshape(shards, local_waves, chunk, both_rows)
        for away in range(1, shards):
            remote(leave_ref, back_ref, out_send, out_recv, away, part).start()
        own(leave_ref, back_ref, 1, part).start()
        return carry

    lax.fori_loop(0, band // chunk, work, 0)

    def finish(part, carry):
        for away in range(1, shards):
            remote(sent_ref, land_ref, in_send, in_recv, away, part).wait_send()
            remote(leave_ref, back_ref, out_send, out_recv, away, part).wait()
        own(leave_ref, back_ref, 1, part).wait()
        return carry

    lax.fori_loop(0, band // chunk, finish, 0)


def cycle_trips(values, wave_ids, points, coef, fields):
    shards, local_waves, band, both_rows = values.shape
    waves = shards * local_waves
    rows = both_rows // 2
    wide = 4 * waves
    lon_max = coef.shape[1]
    chunk = next(c for c in (16, 8) if band % c == 0)
    parts = band // chunk
    lane = jnp.arange(wide)
    part = lane // waves
    wave_lane = jnp.tile(wave_ids, 4).astype(F32)
    factor = jnp.where(wave_lane == 0, 1.0, 2.0)
    own = (part < 2).astype(F32)
    cross = jnp.where(part == 2, -1.0, jnp.where(part == 3, 1.0, 0.0))
    zero = jnp.zeros_like(own)
    lanes = jnp.stack(
        [wave_lane, own * factor, cross * factor, own, -cross, zero, zero, zero], axis=0
    )
    wave_col = jnp.broadcast_to(wave_ids.astype(F32)[:, None], (waves, LOW))
    pick = (jnp.arange(rows)[:, None] == jnp.arange(both_rows)[None, :] % rows).astype(BF16)
    merge = (jnp.arange(waves)[:, None] == jnp.arange(2 * waves)[None, :] % waves).astype(BF16)

    vmem = pl.BlockSpec(memory_space=pltpu.VMEM)
    smem = pl.BlockSpec(memory_space=pltpu.SMEM)
    dma = pltpu.SemaphoreType.DMA
    return pl.pallas_call(
        functools.partial(exchange_kernel, fields, chunk),
        name="cycles",
        out_shape=jax.ShapeDtypeStruct(values.shape, BF16),
        in_specs=[smem, smem] + [vmem] * 6,
        out_specs=vmem,
        scratch_shapes=[
            pltpu.VMEM(values.shape, BF16),
            pltpu.VMEM(values.shape, BF16),
            pltpu.VMEM((chunk, waves, both_rows), F32),
            pltpu.VMEM((chunk, waves, both_rows), F32),
            dma((shards - 1, parts)),
            dma((shards - 1, parts)),
            dma((shards - 1, parts)),
            dma((shards - 1, parts)),
            dma((2, parts)),
        ],
        compiler_params=pltpu.CompilerParams(
            vmem_limit_bytes=30 << 20, collective_id=0, has_side_effects=True
        ),
        cost_estimate=pl.CostEstimate(
            flops=8 * band * waves * rows * lon_max,
            bytes_accessed=4 * band * lon_max,
            transcendentals=0,
        ),
    )(
        points.astype(F32),
        1.0 / points.astype(F32),
        values,
        coef,
        lanes,
        wave_col,
        pick,
        merge,
    )


def level_kernel(
    channels,
    levs,
    ids,
    own_ref,
    in_ref,
    out_modes_ref,
    depth_ref,
    update_ref,
    all_ref,
    far_send,
    far_recv,
    near_send,
    near_recv,
    own_sems,
):
    waves, rows, span = own_ref.shape
    items = rows // channels
    modes = in_ref.shape[0]
    chips = levs // 2
    me = lax.axis_index("lev")
    chip, core = me // 2, lax.rem(me, 2)
    partner = chip * 2 + 1 - core

    barrier = pltpu.get_barrier_semaphore()
    peers = [lax.rem(chip + d, chips) * 2 + core for d in range(1, chips)]
    for peer in peers + [partner]:
        pl.semaphore_signal(
            barrier, inc=1, device_id={"lev": peer}, device_id_type=pl.DeviceIdType.MESH
        )
    pl.semaphore_wait(barrier, chips)

    def far(away, m):
        return pltpu.make_async_remote_copy(
            src_ref=own_ref.at[m],
            dst_ref=all_ref.at[me, m],
            send_sem=far_send.at[away - 1, m],
            recv_sem=far_recv.at[away - 1, m],
            device_id={"lev": peers[away - 1]},
            device_id_type=pl.DeviceIdType.MESH,
        )

    def near(away, m):
        owner = lax.rem(chip + chips - away, chips) * 2 + core
        return pltpu.make_async_remote_copy(
            src_ref=own_ref.at[m] if away == 0 else all_ref.at[owner, m],
            dst_ref=all_ref.at[owner, m],
            send_sem=near_send.at[away, m],
            recv_sem=near_recv.at[away, m],
            device_id={"lev": partner},
            device_id_type=pl.DeviceIdType.MESH,
        )

    def own(m):
        return pltpu.make_async_copy(own_ref.at[m], all_ref.at[me, m], own_sems.at[m])

    for m in range(waves):
        for away in range(1, chips):
            far(away, m).start()
        near(0, m).start()
        own(m).start()

    def solve(m):
        own(m).wait()
        for away in range(chips):
            near(away, m).wait_recv()
        place = lax.broadcasted_iota(jnp.int32, (modes, span), 1)
        degree = (place + ids[m]).astype(F32)
        damp = 1.0 / (1.0 + depth_ref[:, :1] * degree * (degree + 1.0) / float(NT * NT))
        for c in range(channels):
            stack = jnp.concatenate(
                [all_ref[s, m, c * items : (c + 1) * items, :] for s in range(levs)], axis=0
            )
            vals = lax.dot_general(in_ref[...], stack, NN, preferred_element_type=F32)
            scaled = (vals * damp).astype(BF16)
            update_ref[m, c] = lax.dot_general(
                out_modes_ref[...], scaled, NN, preferred_element_type=F32
            ).astype(BF16)

    for m in range(waves):
        for away in range(1, chips):
            far(away, m).wait_recv()
            near(away, m).start()
        if m > 0:
            solve(m - 1)
    solve(waves - 1)
    for m in range(waves):
        for away in range(1, chips):
            far(away, m).wait_send()
        for away in range(chips):
            near(away, m).wait_send()


def vertical(projected, modes_in, own_rows, depths, own_waves, channels, levs):
    waves, rows, span = projected.shape
    items = rows // channels
    modes = modes_in.shape[0]
    chips = levs // 2
    spread = jnp.broadcast_to(depths[:, None], (modes, LANES))
    vmem = pl.BlockSpec(memory_space=pltpu.VMEM)
    dma = pltpu.SemaphoreType.DMA
    return pl.pallas_call(
        functools.partial(level_kernel, channels, levs),
        name="vertical",
        out_shape=jax.ShapeDtypeStruct((waves, channels, items, span), BF16),
        in_specs=[pl.BlockSpec(memory_space=pltpu.SMEM)] + [vmem] * 4,
        out_specs=vmem,
        scratch_shapes=[
            pltpu.VMEM((levs, waves, rows, span), BF16),
            dma((max(chips - 1, 1), waves)),
            dma((max(chips - 1, 1), waves)),
            dma((chips, waves)),
            dma((chips, waves)),
            dma((waves,)),
        ],
        compiler_params=pltpu.CompilerParams(
            vmem_limit_bytes=40 << 20, collective_id=1, has_side_effects=True
        ),
    )(own_waves, projected, modes_in, own_rows, spread)


def on_device(
    spectral,
    legendre,
    wave_ids,
    trunc_lengths,
    cycle_points,
    grid_coef,
    cycle_weights,
    modes_in,
    modes_out,
    depths,
):
    wave_rank = lax.axis_index("wave")
    lev_rank = lax.axis_index("lev")
    shards = lax.axis_size("wave")
    waves, channels, items, span = spectral.shape
    rows = channels * items
    band = grid_coef.shape[0]
    own_waves = lax.dynamic_slice_in_dim(wave_ids, wave_rank * waves, waves)
    own_lengths = lax.dynamic_slice_in_dim(trunc_lengths, wave_rank * waves, waves)
    fourier = inverse_legendre(spectral, legendre, own_lengths, shards)
    points = lax.dynamic_slice_in_dim(cycle_points, wave_rank * band, band)
    returned = cycle_trips(fourier, wave_ids, points, grid_coef, channels // 2)
    projected = forward_legendre(returned, legendre, own_lengths, cycle_weights)
    own_rows = lax.dynamic_slice_in_dim(modes_out, lev_rank * items, items, 0)
    levs = lax.axis_size("lev")
    return vertical(projected, modes_in, own_rows, depths, own_waves, channels, levs)


def solution(mesh):
    placed = (
        P("wave", None, "lev", None),
        P("wave", None, None),
        P(),
        P(),
        P(),
        P("wave", None),
        P(),
        P(),
        P(),
        P(),
    )
    return jax.shard_map(
        on_device,
        mesh=mesh,
        in_specs=placed,
        out_specs=P("wave", None, "lev", None),
        check_vma=False,
    )
```
